8 devices in a mesh: dp: 1 (over z), col: 2 (over y), row: 4 (over x, core).
Axes of the slice: x: 2, y: 2, z: 1, core: 2. Of those that a mesh axis runs over, the one named last changes fastest.
Arguments:
- pair_rep: bfloat16 [1024, 1024, 128], P(('dp', 'row'), 'col')
- pair_mask: int32 [1024, 1024], P(('dp', 'row'), 'col')
- norm_in: bfloat16 [128], replicated
- proj_left: bfloat16 [128, 128], replicated
- gate_left: bfloat16 [128, 128], replicated
- proj_right: bfloat16 [128, 128], replicated
- gate_right: bfloat16 [128, 128], replicated
- proj_gate: bfloat16 [128, 128], replicated
- norm_out: bfloat16 [128], replicated
- proj_out: bfloat16 [128, 128], replicated
Outputs:
- output: bfloat16 [1024, 1024, 128], P(('dp', 'row'), 'col')
All inputs are finite; a program needn't handle non-finite values.
Results may differ from the reference program's by a relative error of at most 0.00618477.
Values are sent between devices in bfloat16 or wider.
A program may use at most 1 GiB of HBM per device.

```python
import jax
import jax.numpy as jnp
from jax import lax

SEQ = 1024
CZ = 128
CHAN = 128
ROW_BLOCK = SEQ // 8
LN_EPS = 1e-5


def layer_norm(values, gain_vec, red_axis):
    centre = values - jnp.mean(values, axis=red_axis, keepdims=True)
    spread = jnp.mean(centre * centre, axis=red_axis, keepdims=True)
    return centre * lax.rsqrt(spread + LN_EPS) * gain_vec


def normal_weight(rng_key, w_shape, std_scale):
    return (jax.random.normal(rng_key, w_shape, jnp.float32) * std_scale).astype(jnp.bfloat16)


def gain_vector(rng_key, gain_width):
    return (1.0 + 0.3 * jax.random.normal(rng_key, (gain_width,), jnp.float32)).astype(jnp.bfloat16)


def setup_inputs(seed: int = 0, part: int = 0) -> dict:
    part_key = jax.random.fold_in(jax.random.key(seed), part)
    pair_key, mask_key = jax.random.split(part_key)
    weight_keys = jax.random.split(jax.random.key(seed + 1), 8)
    pair_rep = jax.random.normal(pair_key, (SEQ, SEQ, CZ), jnp.float32).astype(jnp.bfloat16)
    residue_ok = (jax.random.randint(mask_key, (SEQ,), 0, 10) != 0).astype(jnp.int32)
    pair_mask = residue_ok[:, None] * residue_ok[None, :]
    return dict(
        pair_rep=pair_rep,
        pair_mask=pair_mask,
        norm_in=gain_vector(weight_keys[0], CZ),
        proj_left=normal_weight(weight_keys[1], (CZ, CHAN), CZ ** -0.5),
        gate_left=normal_weight(weight_keys[2], (CZ, CHAN), CZ ** -0.5),
        proj_right=normal_weight(weight_keys[3], (CZ, CHAN), CZ ** -0.5),
        gate_right=normal_weight(weight_keys[4], (CZ, CHAN), CZ ** -0.5),
        proj_gate=normal_weight(weight_keys[5], (CZ, CZ), CZ ** -0.5),
        norm_out=gain_vector(weight_keys[6], CHAN),
        proj_out=normal_weight(weight_keys[7], (CHAN, CZ), 2.0 * CHAN ** -0.5),
    )


def reference(pair_rep, pair_mask, norm_in, proj_left, gate_left, proj_right, gate_right, proj_gate, norm_out, proj_out):
    pair_f = pair_rep.astype(jnp.float32)
    normed = layer_norm(pair_f, norm_in.astype(jnp.float32), -1).astype(jnp.bfloat16)
    flat_x = normed.reshape(SEQ * SEQ, CZ)
    keep_f = pair_mask.astype(jnp.float32).reshape(SEQ * SEQ, 1)

    def gated_proj(w_value, w_gate):
        value_f = jnp.dot(flat_x, w_value, preferred_element_type=jnp.float32)
        gate_vals = jax.nn.sigmoid(jnp.dot(flat_x, w_gate, preferred_element_type=jnp.float32))
        return (keep_f * gate_vals * value_f).astype(jnp.bfloat16).T.reshape(CHAN, SEQ, SEQ)

    left_op = gated_proj(proj_left, gate_left)
    right_op = gated_proj(proj_right, gate_right)
    out_gate = jax.nn.sigmoid(jnp.dot(flat_x, proj_gate, preferred_element_type=jnp.float32))
    gate_blocks = out_gate.reshape(8, ROW_BLOCK, SEQ, CZ)
    left_blocks = left_op.reshape(CHAN, 8, ROW_BLOCK, SEQ).transpose(1, 0, 2, 3)
    pair_blocks = pair_f.reshape(8, ROW_BLOCK, SEQ, CZ)
    gain_out = norm_out.astype(jnp.float32)[:, None, None]

    def channel_product(operands):
        return jnp.dot(operands[0], operands[1].T, preferred_element_type=jnp.float32)

    def row_block(operands):
        left_blk, gate_blk, pair_blk = operands
        contracted = lax.map(channel_product, (left_blk, right_op))
        normed_o = layer_norm(contracted, gain_out, 0).astype(jnp.bfloat16)
        update = jnp.dot(normed_o.reshape(CHAN, ROW_BLOCK * SEQ).T, proj_out, preferred_element_type=jnp.float32)
        return (pair_blk + gate_blk * update.reshape(ROW_BLOCK, SEQ, CZ)).astype(jnp.bfloat16)

    new_pair = lax.map(row_block, (left_blocks, gate_blocks, pair_blocks))
    return new_pair.reshape(SEQ, SEQ, CZ)
```

```python
import functools
import jax, jax.numpy as jnp
from jax import lax
from jax.experimental import pallas as pl
from jax.experimental.pallas import tpu as pltpu
from jax.sharding import PartitionSpec as P
F32, BF16 = jnp.float32, jnp.bfloat16
EPS = 1e-5
def sig(x): return 0.5 * jnp.tanh(0.5 * x) + 0.5

RB = 16
PAD = 24

def front_body(flag_ref, z0_ref, z1_ref, g_ref, w_ref, o_ref, acc):
    K = z0_ref.shape[1]
    gain = jnp.broadcast_to(g_ref[...], (128, K))
    pick = flag_ref[0] != 0
    def row(i, _):
        if z1_ref is None: zi = z0_ref[i]
        else: zi = jnp.where(pick, z0_ref[i], z1_ref[i])
        zt = zi.T.astype(F32)
        c = zt - jnp.mean(zt, axis=0, keepdims=True)
        v = jnp.mean(c * c, axis=0, keepdims=True)
        x = (c * lax.rsqrt(v + EPS) * gain).astype(BF16)
        p = jnp.dot(w_ref[...], x, preferred_element_type=F32)
        ab = sig(p[128:]) * p[:128]
        for t in range(K // 128):
            acc[t, pl.ds(i, 128, stride=PAD), :] = ab[:, t * 128:(t + 1) * 128]
        return 0
    lax.fori_loop(0, RB, row, 0, unroll=2)
    def ch(c, _):
        for t in range(K // 128):
            o_ref[c, :, t * 128:(t + 1) * 128] = acc[t, pl.ds(pl.multiple_of(c * PAD, 8), RB), :].astype(BF16)
        return 0
    lax.fori_loop(0, 128, ch, 0, unroll=8)

def front(flag, z0, z1, g, w):
    R, K, _ = z0.shape
    zspec = lambda which: pl.BlockSpec((RB, K, 128), (lambda i, f: (jnp.where(f[0] != 0, i, 0), 0, 0)) if which == 0 else (lambda i, f: (jnp.where(f[0] != 0, 0, i), 0, 0)))
    if z1 is None:
        body = lambda f, a, gg, ww, o, s: front_body(f, a, None, gg, ww, o, s)
        ins = [pl.BlockSpec((RB, K, 128), lambda i, f: (i, 0, 0))]
        ops = (z0,)
    else:
        body = front_body
        ins = [zspec(0), zspec(1)]
        ops = (z0, z1)
    return pl.pallas_call(body, name="front",
        out_shape=jax.ShapeDtypeStruct((128, R, K), BF16),
        grid_spec=pltpu.PrefetchScalarGridSpec(num_scalar_prefetch=1, grid=(R // RB,),
            in_specs=ins + [pl.BlockSpec((128, 1), lambda i, f: (0, 0)), pl.BlockSpec((256, 128), lambda i, f: (0, 0))],
            out_specs=pl.BlockSpec((128, RB, K), lambda i, f: (0, i, 0)),
            scratch_shapes=[pltpu.VMEM((K // 128, 128 * PAD, 128), F32)]),
        compiler_params=pltpu.CompilerParams(vmem_limit_bytes=60 * 2**20),
        cost_estimate=pl.CostEstimate(flops=R * K * 128 * 256 * 4, bytes_accessed=R * K * 512, transcendentals=R * K * 128),
    )(flag, *ops, g, w)

def gate_body(z_ref, g_ref, w_ref, s_ref):
    def row(i, _):
        z = z_ref[i].astype(F32)
        c = z - jnp.mean(z, axis=1, keepdims=True)
        v = jnp.mean(c * c, axis=1, keepdims=True)
        x = (c * lax.rsqrt(v + EPS) * g_ref[...]).astype(BF16)
        s_ref[i] = sig(jnp.dot(x, w_ref[...], preferred_element_type=F32))
        return 0
    lax.fori_loop(0, z_ref.shape[0], row, 0, unroll=2)

def gate(z, g, w):
    R, K, _ = z.shape
    GB = 8
    return pl.pallas_call(gate_body, name="gate", grid=(R // GB,),
        out_shape=jax.ShapeDtypeStruct((R, K, 128), F32),
        in_specs=[pl.BlockSpec((GB, K, 128), lambda i: (i, 0, 0)), pl.BlockSpec((1, 128), lambda i: (0, 0)), pl.BlockSpec((128, 128), lambda i: (0, 0))],
        out_specs=pl.BlockSpec((GB, K, 128), lambda i: (i, 0, 0)),
        compiler_params=pltpu.CompilerParams(vmem_limit_bytes=60 * 2**20),
        cost_estimate=pl.CostEstimate(flops=R * K * 128 * 128 * 4, bytes_accessed=R * K * 768, transcendentals=R * K * 128),
    )(z, g, w)

CB = 8; IB = 32
def back_body(na, first, me_ref, *refs):
    a_refs = refs[:2 * na]; b0, b1, p0, p1, z_ref, s_ref, g_ref, wo_ref = refs[2 * na:2 * na + 8]
    rest = refs[2 * na + 8:]
    out_ref, o_ref = rest[-2], rest[-1]
    JB = b0.shape[1]; NI = sum(a_refs[i].shape[1] for i in range(na)); ST = o_ref.shape[0] // 128
    t = pl.program_id(0)
    nc = 128 // CB
    dn = (((1,), (1,)), ((), ()))
    @pl.when(t < nc)
    def _():
        for c in range(CB):
            l0 = jnp.concatenate([a_refs[n][c] for n in range(na)], axis=0)
            l1 = jnp.concatenate([a_refs[na + n][c] for n in range(na)], axis=0)
            r0 = jnp.concatenate([b0[c], p0[c]], axis=0)
            r1 = jnp.concatenate([b1[c], p1[c]], axis=0)
            o = lax.dot_general(l0, r0, dn, preferred_element_type=F32) + lax.dot_general(l1, r1, dn, preferred_element_type=F32)
            o_ref[pl.ds(pl.multiple_of((t * CB + c) * ST, 8), NI), :] = o
    @pl.when(t >= nc)
    def _():
        base = (t - nc) * IB
        me = me_ref[0]
        gain = jnp.broadcast_to(g_ref[...], (128, 2 * JB))
        def row(i, _):
            o = o_ref[pl.ds(base + i, 128, stride=ST), :]
            c = o - jnp.mean(o, axis=0, keepdims=True)
            v = jnp.mean(c * c, axis=0, keepdims=True)
            n = (c * lax.rsqrt(v + EPS) * gain).astype(BF16)
            u = lax.dot_general(n, wo_ref[...], (((0,), (0,)), ((), ())), preferred_element_type=F32)
            for grp, lo in ((me, 0), (1 - me, JB)):
                out_ref[i, grp] = (z_ref[i, grp].astype(F32) + s_ref[i, grp] * u[lo:lo + JB]).astype(BF16)
            return 0
        lax.fori_loop(0, IB, row, 0, unroll=2)

def back(me, j0, a0s, a1s, b0, b1, p0, p1, z4, s4, g, wo, prev):
    na = len(a0s); JB, K = b0.shape[1], b0.shape[2]; NI = z4.shape[0]; JT = z4.shape[2]
    nc = 128 // CB
    ST = NI + 8
    jb = j0 // JB
    aspec = [pl.BlockSpec((CB, a.shape[1], K), lambda t, m: (jnp.minimum(t, nc - 1), 0, 0)) for a in list(a0s) + list(a1s)]
    bspec = [pl.BlockSpec((CB, JB, K), lambda t, m: (jnp.minimum(t, nc - 1), 0, 0))] * 4
    pspec = pl.BlockSpec((IB, 2, JB, 128), lambda t, m: (jnp.maximum(t - nc, 0), 0, jb, 0))
    ins = aspec + bspec + [pspec, pspec, pl.BlockSpec((128, 1), lambda t, m: (0, 0)), pl.BlockSpec((128, 128), lambda t, m: (0, 0))]
    ops = [*a0s, *a1s, b0, b1, p0, p1, z4, s4, g, wo]
    al = {}
    if prev is not None:
        ins.append(pl.BlockSpec(memory_space=pl.ANY)); al = {1 + len(ops): 0}; ops.append(prev)
    return pl.pallas_call(functools.partial(back_body, na, prev is None), name="back",
        out_shape=jax.ShapeDtypeStruct(z4.shape, BF16),
        grid_spec=pltpu.PrefetchScalarGridSpec(num_scalar_prefetch=1, grid=(nc + NI // IB,), in_specs=ins, out_specs=pspec,
            scratch_shapes=[pltpu.VMEM((128 * ST, 2 * JB), F32)]),
        input_output_aliases=al,
        compiler_params=pltpu.CompilerParams(vmem_limit_bytes=62 * 2**20),
        cost_estimate=pl.CostEstimate(flops=NI * 2 * JB * 128 * 2 * (2 * K + 256), bytes_accessed=NI * 2048 * 128 + 2 * JB * NI * 1024, transcendentals=0),
    )(me, *ops)


N = 4


def solution(mesh):
    rows, cols = mesh.shape['row'], mesh.shape['col']
    cores = rows // cols
    tile_spec = P(('dp', 'row'), 'col', None)
    mask_spec = P(('dp', 'row'), 'col')
    idx = lambda x, y, c: y * rows + x * cores + c
    both = lambda prs: [(idx(*s, c), idx(*d, c)) for s, d in prs for c in range(cores)]
    swap_y = both([((x, y), (x, 1 - y)) for x in range(2) for y in range(2)])
    send_x = both([((x, x), (1 - x, x)) for x in range(2)])
    send_d = both([((1 - x, x), (x, 1 - x)) for x in range(2)])
    swap_c = [(idx(x, y, c), idx(x, y, 1 - c)) for x in range(2) for y in range(2) for c in range(2)]

    def prog(z, mask, norm_in, proj_left, gate_left, proj_right, gate_right, proj_gate, norm_out, proj_out):
        perm = lambda v, prs: lax.ppermute(v, ('col', 'row'), prs)
        R, K, C = z.shape
        row, col = lax.axis_index('row'), lax.axis_index('col')
        diag = (row // cores == col).astype(jnp.int32)[None]
        me = (row % cores).astype(jnp.int32)[None]
        q = R // N
        tie = lambda v, *deps: lax.optimization_barrier((v,) + deps)[0]
        gin = norm_in.astype(F32)
        gi, go = gin[:, None], norm_out.astype(F32)[:, None]
        wl = jnp.concatenate([proj_left, gate_left], 1).T
        wr = jnp.concatenate([proj_right, gate_right], 1).T
        z4 = z.reshape(R, 2, K // 2, C)
        zc = []
        for n in range(N):
            zn, mn = z[n * q:(n + 1) * q], mask[n * q:(n + 1) * q]
            if n:
                mn = tie(mn, zc[-1])
            zc.append(jnp.where(mn[:, :, None] != 0, zn, jnp.zeros((), BF16)))
        zy = [perm(zc[n], swap_y) for n in range(N)]
        zx, zo, a0, a1 = [None] * N, [None] * N, [], []
        b0, b1, p0, p1 = [None] * N, [None] * N, [None] * N, [None] * N
        zx[0], zx[1] = perm(zc[0], send_x), perm(zc[1], send_x)
        last = [s := gate(tie(z, zc[3]), gin[None], proj_gate)]
        s4 = s.reshape(R, 2, K // 2, C)

        def run(flag, za, zb, w):
            last[0] = front(tie(flag, last[0]), za, zb, gi, w)
            return last[0]

        def right(n, h):
            if h == 0:
                b0[n] = run(diag, zc[n], zx[n], wr)
                p0[n] = perm(b0[n], swap_c)
            else:
                b1[n] = run(diag, zy[n], zo[n], wr)
                p1[n] = perm(b1[n], swap_c)

        def finish(n, out):
            last[0] = back(tie(me, last[0]), n * q, a0, a1, b0[n], b1[n], p0[n], p1[n], z4, s4, go, proj_out, out)
            return last[0]

        for n in range(N):
            a0.append(run(diag, zc[n], None, wl))
        zo[0] = perm(tie(zy[0], last[0]), send_x)
        a1.append(run(diag, zy[0], None, wl))
        right(0, 0)
        zo[1] = perm(tie(zy[1], last[0]), send_x)
        zx[2], zx[3] = perm(tie(zc[2], zy[1], last[0]), send_x), perm(tie(zc[3], zy[1], last[0]), send_x)
        a1.append(run(diag, zy[1], None, wl))
        right(1, 0)
        a1.append(run(diag, zy[2], None, wl))
        right(0, 1)
        zo[2], zo[3] = perm(tie(zc[2], zy[3], last[0]), send_d), perm(tie(zc[3], zy[3], last[0]), send_d)
        a1.append(run(diag, zy[3], None, wl))
        right(1, 1)
        out = finish(0, None)
        out = finish(1, out)
        right(2, 0)
        right(2, 1)
        out = finish(2, out)
        right(3, 0)
        right(3, 1)
        out = finish(3, out)
        return out.reshape(R, K, C)

    return jax.shard_map(prog, mesh=mesh, in_specs=(tile_spec, mask_spec) + (P(),) * 8, out_specs=tile_spec, check_vma=False)
```

```python
import functools
import jax, jax.numpy as jnp
from jax import lax
from jax.experimental import pallas as pl
from jax.experimental.pallas import tpu as pltpu
from jax.sharding import PartitionSpec as P
F32, BF16 = jnp.float32, jnp.bfloat16
EPS = 1e-5
def sig(x): return 0.5 * jnp.tanh(0.5 * x) + 0.5

RB = 16
PAD = 24

def front_body(flag_ref, z0_ref, z1_ref, g_ref, w_ref, o_ref, acc):
    K = z0_ref.shape[1]
    gain = jnp.broadcast_to(g_ref[...], (128, K))
    pick = flag_ref[0] != 0

    def row(i, _):
        if z1_ref is None: zi = z0_ref[i]
        else: zi = jnp.where(pick, z0_ref[i], z1_ref[i])
        zt = zi.T.astype(F32)
        c = zt - jnp.mean(zt, axis=0, keepdims=True)
        v = jnp.mean(c * c, axis=0, keepdims=True)
        x = (c * lax.rsqrt(v + EPS) * gain).astype(BF16)
        p = jnp.dot(w_ref[...], x, preferred_element_type=F32)
        ab = sig(p[128:]) * p[:128]
        for t in range(K // 128):
            acc[t, pl.ds(i, 128, stride=PAD), :] = ab[:, t * 128:(t + 1) * 128]
        return 0

    lax.fori_loop(0, RB, row, 0, unroll=4)

    def ch(c, _):
        for t in range(K // 128):
            o_ref[c, :, t * 128:(t + 1) * 128] = acc[t, pl.ds(pl.multiple_of(c * PAD, 8), RB), :].astype(BF16)
        return 0

    lax.fori_loop(0, 128, ch, 0, unroll=8)

def front(flag, z0, z1, g, w, off=0):
    R, K, _ = (z0 if z1 is None else z1).shape
    ob = off // RB
    zspec = lambda which: pl.BlockSpec((RB, K, 128), (lambda i, f: (jnp.where(f[0] != 0, i + ob, ob), 0, 0)) if which == 0 else (lambda i, f: (jnp.where(f[0] != 0, 0, i), 0, 0)))
    if z1 is None:
        body = lambda f, a, gg, ww, o, s: front_body(f, a, None, gg, ww, o, s)
        ins = [pl.BlockSpec((RB, K, 128), lambda i, f: (i, 0, 0))]
        ops = (z0,)
    else:
        body = front_body
        ins = [zspec(0), zspec(1)]
        ops = (z0, z1)
    return pl.pallas_call(body, name="front",
        out_shape=jax.ShapeDtypeStruct((128, R, K), BF16),
        grid_spec=pltpu.PrefetchScalarGridSpec(num_scalar_prefetch=1, grid=(R // RB,),
            in_specs=ins + [pl.BlockSpec((128, 1), lambda i, f: (0, 0)), pl.BlockSpec((256, 128), lambda i, f: (0, 0))],
            out_specs=pl.BlockSpec((128, RB, K), lambda i, f: (0, i, 0)),
            scratch_shapes=[pltpu.VMEM((K // 128, 128 * PAD, 128), F32)]),
        compiler_params=pltpu.CompilerParams(vmem_limit_bytes=60 * 2**20),
        cost_estimate=pl.CostEstimate(flops=R * K * 128 * 256 * 4, bytes_accessed=R * K * 512, transcendentals=R * K * 128),
    )(flag, *ops, g, w)

def gate_body(z_ref, g_ref, w_ref, s_ref):
    def row(i, _):
        z = z_ref[i].astype(F32)
        c = z - jnp.mean(z, axis=1, keepdims=True)
        v = jnp.mean(c * c, axis=1, keepdims=True)
        x = (c * lax.rsqrt(v + EPS) * g_ref[...]).astype(BF16)
        s_ref[i] = sig(jnp.dot(x, w_ref[...], preferred_element_type=F32))
        return 0

    lax.fori_loop(0, z_ref.shape[0], row, 0, unroll=4)

def gate(z, g, w):
    R, K, _ = z.shape
    GB = 8
    return pl.pallas_call(gate_body, name="gate", grid=(R // GB,),
        out_shape=jax.ShapeDtypeStruct((R, K, 128), F32),
        in_specs=[pl.BlockSpec((GB, K, 128), lambda i: (i, 0, 0)), pl.BlockSpec((1, 128), lambda i: (0, 0)), pl.BlockSpec((128, 128), lambda i: (0, 0))],
        out_specs=pl.BlockSpec((GB, K, 128), lambda i: (i, 0, 0)),
        compiler_params=pltpu.CompilerParams(vmem_limit_bytes=60 * 2**20),
        cost_estimate=pl.CostEstimate(flops=R * K * 128 * 128 * 4, bytes_accessed=R * K * 768, transcendentals=R * K * 128),
    )(z, g, w)


def back_body(na, nb, cb, me_ref, *refs):
    a = [refs[:na], refs[na:2 * na]]
    refs = refs[2 * na:]
    b = [refs[q * nb:(q + 1) * nb] for q in range(4)]
    z_ref, s_ref, g_ref, wo_ref = refs[4 * nb:4 * nb + 4]
    out_ref, o_ref = refs[-2], refs[-1]
    G, IB, _, JB, _ = out_ref.shape
    T, ST = o_ref.shape[0], o_ref.shape[1] // 128
    t = pl.program_id(0)
    nc = 128 // cb
    dn = (((1,), (1,)), ((), ()))

    @pl.when(t < nc)
    def _():
        for c in range(cb):
            o = None
            for h in range(2):
                lhs = jnp.concatenate([r[c] for r in a[h]], axis=0)
                rhs = jnp.concatenate([r[c] for r in b[h]] + [r[c] for r in b[2 + h]], axis=0)
                d = lax.dot_general(lhs, rhs, dn, preferred_element_type=F32)
                o = d if o is None else o + d
            n = o.shape[0] // G
            o = jnp.concatenate([o[q * n:(q + 1) * n] for q in range(G)], axis=1)
            for q in range(T):
                o_ref[q, pl.ds(pl.multiple_of((t * cb + c) * ST, 8), n), :] = o[:, q * 128:(q + 1) * 128]

    @pl.when(t >= nc)
    def _():
        base = (t - nc) * IB
        me = me_ref[0]
        gain = jnp.broadcast_to(g_ref[...], (128, 128))

        def row(i, _):
            u = []
            for q in range(T):
                o = o_ref[q, pl.ds(base + i, 128, stride=ST), :]
                c = o - jnp.mean(o, axis=0, keepdims=True)
                v = jnp.mean(c * c, axis=0, keepdims=True)
                n = (c * lax.rsqrt(v + EPS) * gain).astype(BF16)
                u.append(lax.dot_general(n, wo_ref[...], (((0,), (0,)), ((), ())), preferred_element_type=F32))
            u = jnp.concatenate(u, axis=0)
            for q in range(G):
                for grp, lo in ((me, 2 * q * JB), (1 - me, 2 * q * JB + JB)):
                    out_ref[q, i, grp] = (z_ref[q, i, grp].astype(F32) + s_ref[q, i, grp] * u[lo:lo + JB]).astype(BF16)
            return 0

        lax.fori_loop(0, IB, row, 0, unroll=8 // T)


def back(me, j0, a, b, z, s, g, wo, prev):
    na, nb = len(a[0]), len(b[0])
    JB, K = sum(v.shape[1] for v in b[0]), b[0][0].shape[2]
    R, KT, C = z.shape
    G, T = max(1, 64 // JB), max(1, 2 * JB // 128)
    cb = 8 // T
    IB = 32 // G // T
    nc, nr = 128 // cb, R // G
    ST = nr + 8
    view = (G, nr, 2, KT // 2, C)
    first = lambda t, m: (jnp.minimum(t, nc - 1), 0, 0)
    arrs = [*a[0], *a[1], *b[0], *b[1], *b[2], *b[3]]
    ins = [pl.BlockSpec((cb, v.shape[1], K), first) for v in arrs]
    pspec = pl.BlockSpec((G, IB, 2, JB, C), lambda t, m: (0, jnp.maximum(t - nc, 0), 0, j0 // JB, 0))
    ins += [pspec, pspec, pl.BlockSpec((128, 1), lambda t, m: (0, 0)), pl.BlockSpec((128, 128), lambda t, m: (0, 0))]
    ops = [*arrs, z.reshape(view), s.reshape(view), g, wo]
    al = {}
    if prev is not None:
        ins.append(pl.BlockSpec(memory_space=pl.ANY))
        al = {1 + len(ops): 0}
        ops.append(prev.reshape(view))
    return pl.pallas_call(functools.partial(back_body, na, nb, cb), name="back",
        out_shape=jax.ShapeDtypeStruct(view, BF16),
        grid_spec=pltpu.PrefetchScalarGridSpec(num_scalar_prefetch=1, grid=(nc + nr // IB,), in_specs=ins, out_specs=pspec,
            scratch_shapes=[pltpu.VMEM((T, 128 * ST, 128), F32)]),
        input_output_aliases=al,
        compiler_params=pltpu.CompilerParams(vmem_limit_bytes=62 * 2**20),
        cost_estimate=pl.CostEstimate(flops=R * 2 * JB * 128 * 2 * (2 * K + 256), bytes_accessed=R * 2048 * 128 + 2 * JB * R * 1024, transcendentals=0),
    )(me, *ops).reshape(R, KT, C)


YC = (64, 64, 64, 64)
BC = (64, 64, 64, 32, 32)


def solution(mesh):
    rows, cols = mesh.shape['row'], mesh.shape['col']
    cores = rows // cols
    tile_spec = P(('dp', 'row'), 'col', None)
    mask_spec = P(('dp', 'row'), 'col')
    idx = lambda x, y, c: y * rows + x * cores + c
    both = lambda prs: [(idx(*s, c), idx(*d, c)) for s, d in prs for c in range(cores)]
    swap_y = both([((x, y), (x, 1 - y)) for x in range(2) for y in range(2)])
    send_x = both([((x, x), (1 - x, x)) for x in range(2)])
    send_d = both([((1 - x, x), (x, 1 - x)) for x in range(2)])
    swap_c = [(idx(x, y, c), idx(x, y, 1 - c)) for x in range(2) for y in range(2) for c in range(2)]

    def body(z, mask, norm_in, proj_left, gate_left, proj_right, gate_right, proj_gate, norm_out, proj_out):
        def perm(v, prs):
            return lax.ppermute(v, ('col', 'row'), prs)

        tie = lambda v, *deps: lax.optimization_barrier((v,) + deps)[0]
        row, col = lax.axis_index('row'), lax.axis_index('col')
        diag = (row // cores == col).astype(jnp.int32)[None]
        me = (row % cores).astype(jnp.int32)[None]
        gin = norm_in.astype(F32)
        gi, go = gin[:, None], norm_out.astype(F32)[:, None]
        wl = jnp.concatenate([proj_left, gate_left], 1).T
        wr = jnp.concatenate([proj_right, gate_right], 1).T
        ny, nb = len(YC), len(BC)
        yo = [sum(YC[:n]) for n in range(ny)]
        bo = [sum(BC[:n]) for n in range(nb)]
        where = [max(m for m in range(ny) if yo[m] <= bo[n]) for n in range(nb)]
        zc = []
        for n in range(ny):
            zn, mn = z[yo[n]:yo[n] + YC[n]], mask[yo[n]:yo[n] + YC[n]]
            if n:
                mn = tie(mn, zc[-1])
            zc.append(jnp.where(mn[:, :, None] != 0, zn, jnp.zeros((), BF16)))
        part = lambda v, n: v[where[n]] if BC[n] == YC[where[n]] else v[where[n]][bo[n] - yo[where[n]]:bo[n] - yo[where[n]] + BC[n]]
        zy = [perm(zc[n], swap_y) for n in range(ny)]
        zx, zo = [None] * nb, [None] * nb
        b = [[None] * nb for _ in range(4)]
        a = [[], []]
        zx[0], zx[1] = perm(zc[0], send_x), perm(zc[1], send_x)
        s = gate(z, gin[None], proj_gate)

        def run(flag, za, zb, w, off=0):
            return front(flag, za, zb, gi, w, off)

        def right(n, h):
            za, zb = ((zc, zx), (zy, zo))[h]
            m = where[n]
            b[h][n] = run(diag, za[m], zb[n], wr, bo[n] - yo[m])
            b[2 + h][n] = perm(b[h][n], swap_c)

        def left(n, h):
            a[h].append(run(diag, (zc, zy)[h][n], None, wl))

        def finish(ns, out):
            return back(me, bo[ns[0]], a, [[v[n] for n in ns] for v in b], z, s, go, proj_out, out)

        for n in range(ny):
            left(n, 0)
        zo[0] = perm(zy[0], send_x)
        left(0, 1)
        right(0, 0)
        zo[1] = perm(zy[1], send_x)
        for n in range(2, nb):
            zx[n] = perm(part(zc, n), send_x)
        left(1, 1)
        right(1, 0)
        left(2, 1)
        right(0, 1)
        for n in range(2, nb):
            zo[n] = perm(part(zc, n), send_d)
        right(1, 1)
        left(3, 1)
        out = finish((0, 1), None)
        for n in range(2, nb):
            right(n, 0)
            right(n, 1)
            out = finish((n,), out)
        return out

    return jax.shard_map(body, mesh=mesh, in_specs=(tile_spec, mask_spec) + (P(),) * 8, out_specs=tile_spec, check_vma=False)
```
